32 devices in a mesh: row: 4 (over z), col: 8 (over y, x, core).
Axes of the slice: x: 2, y: 2, z: 4, core: 2. Of those that a mesh axis runs over, the one named last changes fastest.
Arguments:
- diag_blocks: float32 [8, 16, 512, 512], P('row', 'col'), may hold values from -4 to 16, as said below
- horizontal: bfloat16 [8, 16, 512, 512], P('row', 'col'), may hold values from -0.125 to 0.125
- vertical: bfloat16 [8, 16, 512, 512], P('row', 'col'), may hold values from -0.125 to 0.125
Outputs:
- red_factor: float32 [8, 8, 512, 512], P('row', 'col')
- black_schur: float32 [8, 8, 512, 512], P('row', 'col')
- black_links: bfloat16 [8, 8, 4, 512, 512], P('row', 'col')
The draws below stay inside these ranges and needn't reach their ends.
Inputs may be any that keep to these rules, and one draw needn't show every extreme that they name: `diag_blocks`: every block is symmetric and its eigenvalues are at least 1.
All inputs are finite; a program needn't handle non-finite values.
Results may differ from the reference program's by a relative error of at most 0.0054.
Values may be sent and summed in bfloat16 or wider, within the bound.
A program may use at most 128 MiB of HBM per device.

```python
import math
import jax
import jax.numpy as jnp
from jax import lax

BLOCK = 512
GRID_ROWS = 8
GRID_COLS = 16


def draw_diag_blocks(key, part):
    first_key = jax.random.fold_in(key, 11)
    second_key = jax.random.fold_in(key, 12)
    factor = jax.random.normal(first_key, (GRID_ROWS, GRID_COLS, BLOCK, BLOCK), jnp.float32)
    levels = jnp.exp(jax.random.uniform(second_key, (GRID_ROWS, GRID_COLS, BLOCK), jnp.float32, 0.0, math.log(4.0)))
    strength = 2.0
    gram = jnp.einsum('rcik,rcjk->rcij', factor, factor, precision=lax.Precision.HIGHEST) * (strength / BLOCK)
    return gram + levels[..., None] * jnp.eye(BLOCK, dtype=jnp.float32)


def block_levels(rng, dims, split, smallest, top_value):
    def one(position, parts):
        heights = jax.random.uniform(jax.random.fold_in(jax.random.fold_in(rng, 6), position), (parts,), jnp.float32, smallest / len(split), top_value / len(split))
        return jnp.repeat(jnp.exp(heights), dims[position] // parts).reshape((-1,) + (1,) * (len(dims) - position - 1))

    level = one(*split[0])
    for cut in split[1:]:
        level = level * one(*cut)
    return level


def gaussian(rng, shape, width, most, pieces=(), kind=jnp.bfloat16):
    factor_of = block_levels(rng, shape, pieces, -0.22, 0.18) if pieces else 1.0
    drawn = jax.random.normal(rng, shape, jnp.float32) * width * factor_of
    return jnp.minimum(jnp.maximum(drawn, -most), most).astype(kind)


def setup_inputs(seed: int = 0) -> dict:
    keys = jax.random.split(jax.random.key(seed), 4)
    diag_blocks = draw_diag_blocks(jax.random.fold_in(keys[3], 71), 0)
    horizontal = gaussian(keys[1], (GRID_ROWS, GRID_COLS, BLOCK, BLOCK), (4 * BLOCK) ** -0.5, 0.125, ((0, 4), (1, 8)))
    vertical = gaussian(keys[2], (GRID_ROWS, GRID_COLS, BLOCK, BLOCK), (4 * BLOCK) ** -0.5, 0.125, ((0, 4), (1, 8)))
    return dict(diag_blocks=diag_blocks, horizontal=horizontal, vertical=vertical)


def select_colour(blocks, parity):
    grid_rows = blocks.shape[0]
    grid_columns = blocks.shape[1]
    trailing = blocks.shape[2:]
    paired = blocks.reshape((grid_rows // 2, 2, grid_columns // 2, 2) + trailing)
    joined = jnp.stack([paired[:, 0, :, parity], paired[:, 1, :, 1 - parity]], 1)
    return joined.reshape((grid_rows, grid_columns // 2) + trailing)

def combine_rows(even_rows, odd_rows):
    joined = jnp.stack([even_rows, odd_rows], 1)
    return joined.reshape((2 * even_rows.shape[0],) + even_rows.shape[1:])

def transposed(blocks):
    return jnp.swapaxes(blocks, -1, -2)

def gram_term(former, latter):
    return jnp.einsum('mka,mkb->mab', former.astype(jnp.float32), latter.astype(jnp.float32), precision=lax.Precision.HIGHEST)

def solve_red(packed):
    factor = jnp.linalg.cholesky(packed[0])
    results = [jax.scipy.linalg.solve_triangular(factor, coupling, lower=True) for coupling in packed[1:]]
    return (factor, jnp.stack(results, 1).astype(jnp.bfloat16))

def black_row(packed):
    diag_black, above, below, left_red, right_red = packed
    update = gram_term(above[:, 3], above[:, 3]) + gram_term(below[:, 1], below[:, 1])
    update = update + gram_term(left_red[:, 2], left_red[:, 2]) + gram_term(right_red[:, 0], right_red[:, 0])
    schur_part = diag_black - update
    east_link = -gram_term(right_red[:, 0], right_red[:, 2])
    south_link = -gram_term(below[:, 1], below[:, 3])
    southeast = -(gram_term(right_red[:, 0], right_red[:, 3]) + gram_term(below[:, 1], below[:, 2]))
    southwest = -(gram_term(left_red[:, 2], left_red[:, 3]) + gram_term(below[:, 1], below[:, 0]))
    links = jnp.stack([east_link, south_link, southeast, southwest], 1).astype(jnp.bfloat16)
    return (schur_part, links)

def reference(diag_blocks, horizontal, vertical):
    left_links = jnp.roll(horizontal, 1, axis=1)
    upper_links = jnp.roll(vertical, 1, axis=0)
    couplings = (transposed(select_colour(left_links, 0)).astype(jnp.float32), transposed(select_colour(upper_links, 0)).astype(jnp.float32), select_colour(horizontal, 0).astype(jnp.float32), select_colour(vertical, 0).astype(jnp.float32))
    red_factor, solved = lax.map(solve_red, (select_colour(diag_blocks, 0),) + couplings)
    above = jnp.roll(solved, 1, axis=0)
    below = jnp.roll(solved, -1, axis=0)
    previous = jnp.roll(solved, 1, axis=1)
    following = jnp.roll(solved, -1, axis=1)
    left_red = combine_rows(solved[0::2], previous[1::2])
    right_red = combine_rows(following[0::2], solved[1::2])
    black_schur, black_links = lax.map(black_row, (select_colour(diag_blocks, 1), above, below, left_red, right_red))
    return (red_factor, black_schur, black_links)
```

```python
import functools

import jax
import jax.numpy as jnp
from jax import lax
from jax.experimental import pallas as pl
from jax.experimental.pallas import tpu as pltpu
from jax.sharding import PartitionSpec as P

PANEL = 128
STRIP = 16
HALF = 256
MESH = pl.DeviceIdType.MESH
VMEM = pl.BlockSpec(memory_space=pltpu.VMEM)
ANY = pl.BlockSpec(memory_space=pl.ANY)
TN = (((0,), (0,)), ((), ()))


def split(value):
    high = value.astype(jnp.bfloat16)
    low = (value - high.astype(jnp.float32)).astype(jnp.bfloat16)
    return high, low


def product(left, right):
    dot = functools.partial(jnp.dot, preferred_element_type=jnp.float32)
    (lh, ll), (rh, rl) = left, right
    return dot(lh, rh) + (dot(lh, rl) + dot(ll, rh))


def factor_diagonal(work, count):
    lane = lax.broadcasted_iota(jnp.int32, (STRIP, PANEL), 1)
    sub = lax.broadcasted_iota(jnp.int32, (STRIP, PANEL), 0)
    sub_wide = lax.broadcasted_iota(jnp.int32, (STRIP, 2 * PANEL), 0)

    def strip(b, carry):
        start = pl.multiple_of(b * STRIP, STRIP)
        rows = [work[m, pl.ds(start, STRIP), :] for m in range(count)]
        columns = [
            [
                jnp.take_along_axis(rows[m][:, :PANEL], jnp.full_like(lane, start + c), axis=1)
                for c in range(STRIP)
            ]
            for m in range(count)
        ]
        for j in range(STRIP):
            for m in range(count):
                column = columns[m][j]
                pivot = jnp.broadcast_to(column[j : j + 1], column.shape)
                root = lax.rsqrt(pivot)
                square = root * root
                below = jnp.where(sub > j, column, 0.0)
                for c in range(j + 1, STRIP):
                    across = jnp.broadcast_to(columns[m][c][j : j + 1], column.shape)
                    columns[m][c] = columns[m][c] - (below * across) * square
                row = jnp.broadcast_to(rows[m][j : j + 1], rows[m].shape)
                wide_below = jnp.concatenate([below * square] * 2, 1)
                wide_root = jnp.concatenate([root] * 2, 1)
                rows[m] = jnp.where(sub_wide == j, row * wide_root, rows[m] - wide_below * row)
        for m in range(count):
            work[m, pl.ds(start, STRIP), :] = rows[m]
            high = rows[m].astype(jnp.bfloat16).astype(jnp.float32)
            low = rows[m] - high
            after = lane >= start + STRIP
            left_high = jnp.where(after, high[:, :PANEL], 0.0)
            left_low = jnp.where(after, low[:, :PANEL], 0.0)
            left = jnp.concatenate([left_high, left_high, left_low, left_low], 0)
            right = jnp.concatenate([high, low, high, low], 0)
            work[m] = work[m] - lax.dot_general(
                left.T.astype(jnp.bfloat16),
                right.astype(jnp.bfloat16),
                (((1,), (0,)), ((), ())),
                preferred_element_type=jnp.float32,
            )
        return carry

    lax.fori_loop(0, PANEL // STRIP, strip, 0)


def triangle(order):
    return [(p, q) for p in range(order // PANEL) for q in range(p + 1)]


def factor_reds(blocks, factor, inverse, work, packed):
    count, order = blocks.shape[0], blocks.shape[2]
    row = lax.broadcasted_iota(jnp.int32, (PANEL, PANEL), 0)
    col = lax.broadcasted_iota(jnp.int32, (PANEL, PANEL), 1)
    eye = jnp.where(row == col, 1.0, 0.0).astype(jnp.float32)
    inverse[...] = jnp.zeros_like(inverse)
    factor[...] = jnp.zeros_like(factor)
    for start in range(0, order, PANEL):
        stop = start + PANEL
        here = slice(start, stop)
        for m in range(count):
            work[m, :, :PANEL] = blocks[m, here, here]
            work[m, :, PANEL:] = eye
        factor_diagonal(work, count)
        for m in range(count):
            upper = jnp.where(col >= row, work[m, :, :PANEL], 0.0)
            factor[m, here, here] = upper.T
            small = jnp.where(col <= row, work[m, :, PANEL:], 0.0)
            small_parts = split(small)
            if start:
                inverse[m, here, :start] = product(small_parts, split(inverse[m, here, :start]))
            inverse[m, here, here] = small
            if stop < order:
                across = product(small_parts, split(blocks[m, here, stop:]))
                down = across.T
                factor[m, stop:, here] = down
                down_parts = split(down)
                blocks[m, stop:, stop:] -= product(down_parts, split(across))
                inverse[m, stop:, :stop] -= product(down_parts, split(inverse[m, here, :stop]))
    for m in range(count):
        for n, (p, q) in enumerate(triangle(order)):
            tile = inverse[m, p * PANEL : (p + 1) * PANEL, q * PANEL : (q + 1) * PANEL]
            packed[m, n] = tile.astype(jnp.bfloat16)


def solve(packed, coupling, flipped, out):
    order = coupling.shape[0]
    axes = (((1,), (1 if flipped else 0,)), ((), ()))
    n = 0
    for p in range(order // PANEL):
        tiles = [packed[n + q] for q in range(p + 1)]
        n += p + 1
        stop = (p + 1) * PANEL
        left = jnp.concatenate(tiles, 1) if p else tiles[0]
        right = coupling[:, :stop] if flipped else coupling[:stop, :]
        value = lax.dot_general(left, right, axes, preferred_element_type=jnp.float32)
        out[p * PANEL : stop, :] = value.astype(jnp.bfloat16)


def grams(order, terms):
    def body(step, carry):
        rows = pl.ds(pl.multiple_of(step * HALF, HALF), HALF)
        for pairs, emit in terms:
            total = None
            for left, right in pairs:
                value = lax.dot_general(
                    left[:, rows], right[...], TN, preferred_element_type=jnp.float32
                )
                total = value if total is None else total + value
            emit(rows, total)
        return carry

    lax.fori_loop(0, order // HALF, body, 0)


def symmetric_tiles(solved, packed):
    order = solved.shape[0]
    n = 0
    for p in range(order // PANEL):
        stop = (p + 1) * PANEL
        value = lax.dot_general(
            solved[:, p * PANEL : stop],
            solved[:, :stop],
            TN,
            preferred_element_type=jnp.float32,
        )
        for q in range(p + 1):
            packed[n] = value[:, q * PANEL : (q + 1) * PANEL].astype(jnp.bfloat16)
            n += 1


def subtract_symmetric(packed, out):
    for n, (p, q) in enumerate(triangle(out.shape[0])):
        rows = slice(p * PANEL, (p + 1) * PANEL)
        cols = slice(q * PANEL, (q + 1) * PANEL)
        tile = packed[n].astype(jnp.float32)
        out[rows, cols] -= tile
        if p != q:
            out[cols, rows] -= tile.T


def subtract_into(out):
    def emit(rows, total):
        out[rows, :] -= total

    return emit


def negate_into(out):
    def emit(rows, total):
        out[rows, :] = (-total).astype(jnp.bfloat16)

    return emit


def negate_with(extra, out):
    def emit(rows, total):
        out[rows, :] = (-(total + extra[rows, :].astype(jnp.float32))).astype(jnp.bfloat16)

    return emit


def whole_kernel(
    diag, hor, ver,
    factor, schur, links,
    blocks, inverse, work, packed, flat, upright,
    from_up, from_right, inv_up, inv_right, own, own_right, near, near_up,
    give_sym, give_cross, got_left_sym, got_left_cross, got_above,
    local, send, recv,
):
    order = blocks.shape[1]
    r, c = lax.axis_index("row"), lax.axis_index("col")
    rows, cols = lax.axis_size("row"), lax.axis_size("col")
    above, beneath = lax.rem(r + rows - 1, rows), lax.rem(r + 1, rows)
    left, right = lax.rem(c + cols - 1, cols), lax.rem(c + 1, cols)
    loads = [
        pltpu.make_async_copy(diag.at[0, 0], blocks.at[0], local.at[0]),
        pltpu.make_async_copy(diag.at[1, 1], blocks.at[1], local.at[1]),
        pltpu.make_async_copy(diag.at[0, 1], schur.at[0], local.at[2]),
        pltpu.make_async_copy(diag.at[1, 0], schur.at[1], local.at[3]),
        pltpu.make_async_copy(hor, flat, local.at[4]),
        pltpu.make_async_copy(ver, upright, local.at[5]),
    ]
    barrier = pltpu.get_barrier_semaphore()
    peers = [(above, c), (beneath, c), (r, left), (r, right), (above, right), (beneath, left)]
    for peer in peers:
        pl.semaphore_signal(barrier, inc=1, device_id=peer, device_id_type=MESH)
    for load in loads:
        load.start()
    pl.semaphore_wait(barrier, len(peers))

    def remote(src, dst, k, peer):
        copy = pltpu.make_async_remote_copy(
            src_ref=src, dst_ref=dst, send_sem=send.at[k], recv_sem=recv.at[k],
            device_id=peer, device_id_type=MESH,
        )
        copy.start()
        return copy

    sent = [
        remote(ver.at[0, 0], from_up.at[0], 0, (above, c)),
        remote(hor.at[0, 0], from_up.at[1], 1, (above, c)),
        remote(hor.at[0, 1], from_up.at[2], 2, (above, right)),
        remote(ver.at[0, 0], from_right.at[0], 3, (r, left)),
        remote(hor.at[0, 0], from_right.at[1], 4, (r, left)),
    ]
    loads[0].wait()
    loads[1].wait()
    factor_reds(blocks, factor, inverse, work, packed)
    for load in loads[2:]:
        load.wait()
    U, L, D, R = (slice(k * order, (k + 1) * order) for k in range(4))
    for at, coupling, flipped in (
        (D, upright.at[1, 1], False),
        (R, flat.at[1, 1], False),
    ):
        solve(packed.at[1], coupling, flipped, own.at[:, at])
    sent.append(remote(packed.at[0], inv_up, 5, (above, c)))
    sent.append(remote(packed.at[0], inv_right, 6, (r, left)))
    symmetric_tiles(own.at[:, D], give_sym.at[0])
    symmetric_tiles(own.at[:, R], give_sym.at[1])

    def give(rows, total):
        give_cross[rows, :] = total.astype(jnp.bfloat16)

    grams(order, [([(own.at[:, R], own.at[:, D])], give)])
    solve(packed.at[1], upright.at[0, 1], True, own.at[:, U])
    sent.append(remote(give_sym.at[0], got_above, 7, (beneath, c)))
    sent.append(remote(give_sym.at[1], got_left_sym, 8, (r, right)))
    sent.append(remote(give_cross, got_left_cross, 9, (r, right)))
    solve(packed.at[1], flat.at[1, 0], True, own.at[:, L])
    first, second = slice(0, order), slice(order, 2 * order)
    solve(packed.at[0], upright.at[0, 0], False, own_right.at[:, first])
    solve(packed.at[0], flat.at[0, 0], False, own_right.at[:, second])
    down, across = own_right.at[:, first], own_right.at[:, second]
    up_, left_, down_, right_ = (own.at[:, at] for at in (U, L, D, R))
    grams(
        order,
        [
            ([(across, across), (up_, up_)], subtract_into(schur.at[0])),
            ([(up_, down_)], negate_into(links.at[0, 1])),
            ([(across, down), (up_, left_)], negate_into(links.at[0, 3])),
            ([(down, down), (left_, left_)], subtract_into(schur.at[1])),
            ([(left_, right_)], negate_into(links.at[1, 0])),
        ],
    )
    sent[3].wait_recv()
    sent[4].wait_recv()
    sent[6].wait_recv()
    near_left, near_down, near_right = (near.at[:, k * order : (k + 1) * order] for k in range(3))
    solve(inv_right, flat.at[0, 1], True, near_left)
    solve(inv_right, from_right.at[0], False, near_down)
    solve(inv_right, from_right.at[1], False, near_right)
    grams(
        order,
        [
            ([(near_left, near_left)], subtract_into(schur.at[0])),
            ([(near_left, near_right)], negate_into(links.at[0, 0])),
            ([(up_, right_), (near_left, near_down)], negate_into(links.at[0, 2])),
        ],
    )
    sent[8].wait_recv()
    subtract_symmetric(got_left_sym, schur.at[1])
    sent[9].wait_recv()
    sent[0].wait_recv()
    sent[1].wait_recv()
    sent[2].wait_recv()
    sent[5].wait_recv()
    below_up, below_left, below_down, below_right = (near_up.at[:, at] for at in (U, L, D, R))
    solve(inv_up, upright.at[1, 0], True, below_up)
    solve(inv_up, from_up.at[2], True, below_left)
    solve(inv_up, from_up.at[0], False, below_down)
    solve(inv_up, from_up.at[1], False, below_right)
    grams(
        order,
        [
            ([(below_up, below_up)], subtract_into(schur.at[1])),
            ([(below_up, below_down)], negate_into(links.at[1, 1])),
            ([(left_, down_), (below_up, below_right)], negate_into(links.at[1, 2])),
            ([(below_up, below_left)], negate_with(got_left_cross, links.at[1, 3])),
        ],
    )
    sent[7].wait_recv()
    subtract_symmetric(got_above, schur.at[0])
    for copy in sent:
        copy.wait_send()


def on_device(diag_blocks, horizontal, vertical):
    order = diag_blocks.shape[-1]
    assert diag_blocks.shape[:2] == (2, 2)
    tiles = len(triangle(order))
    square = (order, order)
    bf16, f32 = jnp.bfloat16, jnp.float32
    packed = (tiles, PANEL, PANEL)
    factor, schur, links = pl.pallas_call(
        whole_kernel,
        out_shape=(
            jax.ShapeDtypeStruct((2,) + square, f32),
            jax.ShapeDtypeStruct((2,) + square, f32),
            jax.ShapeDtypeStruct((2, 4) + square, bf16),
        ),
        in_specs=[ANY] * 3,
        out_specs=(VMEM, VMEM, VMEM),
        scratch_shapes=[
            pltpu.VMEM((2,) + square, f32),
            pltpu.VMEM((2,) + square, f32),
            pltpu.VMEM((2, PANEL, 2 * PANEL), f32),
            pltpu.VMEM((2,) + packed, bf16),
            pltpu.VMEM((2, 2) + square, bf16),
            pltpu.VMEM((2, 2) + square, bf16),
            pltpu.VMEM((3,) + square, bf16),
            pltpu.VMEM((2,) + square, bf16),
            pltpu.VMEM(packed, bf16),
            pltpu.VMEM(packed, bf16),
            pltpu.VMEM((order, 4 * order), bf16),
            pltpu.VMEM((order, 2 * order), bf16),
            pltpu.VMEM((order, 3 * order), bf16),
            pltpu.VMEM((order, 4 * order), bf16),
            pltpu.VMEM((2,) + packed, bf16),
            pltpu.VMEM(square, bf16),
            pltpu.VMEM(packed, bf16),
            pltpu.VMEM(square, bf16),
            pltpu.VMEM(packed, bf16),
            pltpu.SemaphoreType.DMA((6,)),
            pltpu.SemaphoreType.DMA((10,)),
            pltpu.SemaphoreType.DMA((10,)),
        ],
        compiler_params=pltpu.CompilerParams(
            collective_id=0, has_side_effects=True, vmem_limit_bytes=44 * 2**20
        ),
        cost_estimate=pl.CostEstimate(
            flops=20_000_000_000, bytes_accessed=8 * diag_blocks.size, transcendentals=0
        ),
    )(diag_blocks, horizontal, vertical)
    return (factor[:, None], schur[:, None], links[:, None])


def solution(mesh):
    in_specs = (
        P("row", "col", None, None),
        P("row", "col", None, None),
        P("row", "col", None, None),
    )
    out_specs = (
        P("row", "col", None, None),
        P("row", "col", None, None),
        P("row", "col", None, None, None),
    )
    return jax.shard_map(
        on_device, mesh=mesh, in_specs=in_specs, out_specs=out_specs, check_vma=False
    )
```

```python
import functools

import jax
import jax.numpy as jnp
from jax import lax
from jax.experimental import pallas as pl
from jax.experimental.pallas import tpu as pltpu
from jax.sharding import PartitionSpec as P

PANEL = 128
STRIP = 16
HALF = 256
ROW_TILE = 16
MESH = pl.DeviceIdType.MESH
VMEM = pl.BlockSpec(memory_space=pltpu.VMEM)
HBM = pl.BlockSpec(memory_space=pltpu.HBM)
TN = (((0,), (0,)), ((), ()))


def split(value):
    high = value.astype(jnp.bfloat16)
    low = (value - high.astype(jnp.float32)).astype(jnp.bfloat16)
    return high, low


def product(left, right):
    dot = functools.partial(jnp.dot, preferred_element_type=jnp.float32)
    (lh, ll), (rh, rl) = left, right
    return dot(lh, rh) + (dot(lh, rl) + dot(ll, rh))


def factor_diagonal(work, count):
    lane = lax.broadcasted_iota(jnp.int32, (STRIP, PANEL), 1)
    sub = lax.broadcasted_iota(jnp.int32, (STRIP, PANEL), 0)
    sub_wide = lax.broadcasted_iota(jnp.int32, (STRIP, 2 * PANEL), 0)

    def strip(b, carry):
        start = pl.multiple_of(b * STRIP, STRIP)
        rows = [work[m, pl.ds(start, STRIP), :] for m in range(count)]
        columns = [
            [
                jnp.take_along_axis(rows[m][:, :PANEL], jnp.full_like(lane, start + c), axis=1)
                for c in range(STRIP)
            ]
            for m in range(count)
        ]
        for j in range(STRIP):
            for m in range(count):
                column = columns[m][j]
                pivot = jnp.broadcast_to(column[j : j + 1], column.shape)
                root = lax.rsqrt(pivot)
                square = root * root
                below = jnp.where(sub > j, column, 0.0)
                for c in range(j + 1, STRIP):
                    across = jnp.broadcast_to(columns[m][c][j : j + 1], column.shape)
                    columns[m][c] = columns[m][c] - (below * across) * square
                row = jnp.broadcast_to(rows[m][j : j + 1], rows[m].shape)
                wide_below = jnp.concatenate([below * square] * 2, 1)
                wide_root = jnp.concatenate([root] * 2, 1)
                rows[m] = jnp.where(sub_wide == j, row * wide_root, rows[m] - wide_below * row)
        for m in range(count):
            work[m, pl.ds(start, STRIP), :] = rows[m]
            high = rows[m].astype(jnp.bfloat16).astype(jnp.float32)
            low = rows[m] - high
            after = lane >= start + STRIP
            left_high = jnp.where(after, high[:, :PANEL], 0.0)
            left_low = jnp.where(after, low[:, :PANEL], 0.0)
            left = jnp.concatenate([left_high, left_high, left_low, left_low], 0)
            right = jnp.concatenate([high, low, high, low], 0)
            work[m] = work[m] - lax.dot_general(
                left.T.astype(jnp.bfloat16),
                right.astype(jnp.bfloat16),
                (((1,), (0,)), ((), ())),
                preferred_element_type=jnp.float32,
            )
        return carry

    lax.fori_loop(0, PANEL // STRIP, strip, 0)


def triangle(order):
    return [(p, q) for p in range(order // PANEL) for q in range(p + 1)]


def factor_reds(blocks, factor, inverse, work, packed):
    count, order = blocks.shape[0], blocks.shape[2]
    row = lax.broadcasted_iota(jnp.int32, (PANEL, PANEL), 0)
    col = lax.broadcasted_iota(jnp.int32, (PANEL, PANEL), 1)
    eye = jnp.where(row == col, 1.0, 0.0).astype(jnp.float32)
    inverse[...] = jnp.zeros_like(inverse)
    factor[...] = jnp.zeros_like(factor)
    for start in range(0, order, PANEL):
        stop = start + PANEL
        here = slice(start, stop)
        for m in range(count):
            work[m, :, :PANEL] = blocks[m, here, here]
            work[m, :, PANEL:] = eye
        factor_diagonal(work, count)
        for m in range(count):
            upper = jnp.where(col >= row, work[m, :, :PANEL], 0.0)
            factor[m, here, here] = upper.T
            small = jnp.where(col <= row, work[m, :, PANEL:], 0.0)
            small_parts = split(small)
            if start:
                inverse[m, here, :start] = product(small_parts, split(inverse[m, here, :start]))
            inverse[m, here, here] = small
            if stop < order:
                across = product(small_parts, split(blocks[m, here, stop:]))
                down = across.T
                factor[m, stop:, here] = down
                down_parts = split(down)
                blocks[m, stop:, stop:] -= product(down_parts, split(across))
                inverse[m, stop:, :stop] -= product(down_parts, split(inverse[m, here, :stop]))
    for m in range(count):
        for n, (p, q) in enumerate(triangle(order)):
            tile = inverse[m, p * PANEL : (p + 1) * PANEL, q * PANEL : (q + 1) * PANEL]
            packed[m, 0, n], packed[m, 1, n] = split(tile)


def triangle_index(p, q):
    return p * (p + 1) // 2 + q


def off_diagonal(order):
    return [(p, q) for p, q in triangle(order) if p != q]


def grid_of_panel():
    row = lax.broadcasted_iota(jnp.int32, (PANEL, PANEL), 0)
    col = lax.broadcasted_iota(jnp.int32, (PANEL, PANEL), 1)
    return row, col


def compact_rows(order):
    panels = order // PANEL
    return (len(off_diagonal(order)) + panels // 2) * PANEL + ROW_TILE


def tile_rows(n):
    return slice(n * PANEL, (n + 1) * PANEL)


def compact(tile_of, order, out, flip):
    row, col = grid_of_panel()
    pairs = off_diagonal(order)
    for n, (p, q) in enumerate(pairs):
        out[tile_rows(n), :] = tile_of(p, q).astype(jnp.bfloat16)
    lines = []
    for k in range(0, order // PANEL, 2):
        first, second = tile_of(k, k), tile_of(k + 1, k + 1)
        other = second.T if flip else second
        joined = jnp.where(row >= col, first, other)
        out[tile_rows(len(pairs) + k // 2), :] = joined.astype(jnp.bfloat16)
        lines.append(jnp.sum(jnp.where(row == col, second, 0.0), axis=0, keepdims=True))
    lines.append(jnp.zeros((ROW_TILE - len(lines), PANEL), jnp.float32))
    base = compact_rows(order) - ROW_TILE
    out[base:, :] = jnp.concatenate(lines, 0).astype(jnp.bfloat16)


def spread_diagonal(packed, order, symmetric):
    row, col = grid_of_panel()
    skip = len(off_diagonal(order))
    base = compact_rows(order) - ROW_TILE
    lines = packed[base:, :].astype(jnp.float32)
    tiles = []
    for k in range(order // PANEL // 2):
        joined = packed[tile_rows(skip + k), :].astype(jnp.float32)
        turned = joined.T
        line = jnp.broadcast_to(lines[k : k + 1, :], joined.shape)
        tiles.append(jnp.where(row >= col, joined, turned if symmetric else 0.0))
        upper = joined if symmetric else 0.0
        tiles.append(jnp.where(row == col, line, jnp.where(col < row, turned, upper)))
    return tiles


def solve(parts, coupling, flipped, out, columns=None):
    order = out.shape[0]
    axes = (((1,), (1 if flipped else 0,)), ((), ()))
    for p in range(order // PANEL):
        stop = (p + 1) * PANEL
        right = coupling[:, :stop] if flipped else coupling[:stop, :]
        value = None
        for tile_of in parts:
            tiles = [tile_of(p, q) for q in range(p + 1)]
            left = jnp.concatenate(tiles, 1) if p else tiles[0]
            term = lax.dot_general(left, right, axes, preferred_element_type=jnp.float32)
            value = term if value is None else value + term
        out[p * PANEL : stop, :] = value.astype(jnp.bfloat16)


def own_parts(packed, m):
    return [
        lambda p, q, part=part: packed[m, part, triangle_index(p, q)] for part in range(2)
    ]


def far_parts(packed, diagonal, order):
    for k, tile in enumerate(spread_diagonal(packed, order, False)):
        diagonal[k] = tile.astype(jnp.bfloat16)
    place = {pair: n for n, pair in enumerate(off_diagonal(order))}
    return [lambda p, q: diagonal[p] if p == q else packed[tile_rows(place[p, q]), :]]


def grams(order, terms):
    def body(step, carry):
        rows = pl.ds(pl.multiple_of(step * HALF, HALF), HALF)
        for pairs, emit in terms:
            total = None
            for left, right in pairs:
                value = lax.dot_general(
                    left[:, rows], right[...], TN, preferred_element_type=jnp.float32
                )
                total = value if total is None else total + value
            emit(rows, total)
        return carry

    lax.fori_loop(0, order // HALF, body, 0)


def compact_gram(solved, out):
    order = solved.shape[0]
    strips = [
        lax.dot_general(
            solved[:, tile_rows(p)],
            solved[:, : (p + 1) * PANEL],
            TN,
            preferred_element_type=jnp.float32,
        )
        for p in range(order // PANEL)
    ]
    compact(lambda p, q: strips[p][:, tile_rows(q)], order, out, False)


def subtract_compact(packed, out):
    order = out.shape[0]
    for n, (p, q) in enumerate(off_diagonal(order)):
        tile = packed[tile_rows(n), :].astype(jnp.float32)
        out[tile_rows(p), tile_rows(q)] -= tile
        out[tile_rows(q), tile_rows(p)] -= tile.T
    for k, tile in enumerate(spread_diagonal(packed, order, True)):
        out[tile_rows(k), tile_rows(k)] -= tile


def subtract_into(out):
    def emit(rows, total):
        out[rows, :] -= total

    return emit


def negate_into(out):
    def emit(rows, total):
        out[rows, :] = (-total).astype(jnp.bfloat16)

    return emit


def negate_with(extra, out):
    def emit(rows, total):
        out[rows, :] = (-(total + extra[rows, :].astype(jnp.float32))).astype(jnp.bfloat16)

    return emit


def whole_kernel(
    diag, hor, ver,
    factor, schur, links,
    blocks, inverse, work, packed, flat, upright,
    from_up, from_right, mine, inv_up, inv_right, diag_up, diag_right,
    own, own_right, near, near_up,
    give_down, give_sym, give_cross, got_sym, got_cross, got_above,
    local, send, recv,
):
    order = blocks.shape[1]
    half = order // 2
    r, c = lax.axis_index("row"), lax.axis_index("col")
    rows, cols = lax.axis_size("row"), lax.axis_size("col")
    above, beneath = lax.rem(r + rows - 1, rows), lax.rem(r + 1, rows)
    left, right = lax.rem(c + cols - 1, cols), lax.rem(c + 1, cols)
    loads = [
        pltpu.make_async_copy(diag.at[0, 0], blocks.at[0], local.at[0]),
        pltpu.make_async_copy(diag.at[1, 1], blocks.at[1], local.at[1]),
        pltpu.make_async_copy(diag.at[0, 1], schur.at[0], local.at[2]),
        pltpu.make_async_copy(diag.at[1, 0], schur.at[1], local.at[3]),
        pltpu.make_async_copy(hor, flat, local.at[4]),
        pltpu.make_async_copy(ver, upright, local.at[5]),
    ]
    barrier = pltpu.get_barrier_semaphore()
    peers = [(above, c), (beneath, c), (r, left), (r, right), (above, right), (beneath, left)]
    for peer in peers:
        pl.semaphore_signal(barrier, inc=1, device_id=peer, device_id_type=MESH)
    for load in loads:
        load.start()
    pl.semaphore_wait(barrier, len(peers))

    def remote(src, dst, k, peer):
        copy = pltpu.make_async_remote_copy(
            src_ref=src, dst_ref=dst, send_sem=send.at[k], recv_sem=recv.at[k],
            device_id=peer, device_id_type=MESH,
        )
        copy.start()
        return copy

    down_up = remote(ver.at[0, 0], from_up.at[0], 0, (above, c))
    right_up = remote(hor.at[0, 0], from_up.at[1], 1, (above, c))
    left_up = [remote(hor.at[0, 1, :half], from_up.at[2, :half], 2, (above, right))]
    down_right = remote(ver.at[0, 0], from_right.at[0], 3, (r, left))
    right_right = remote(hor.at[0, 0], from_right.at[1], 4, (r, left))
    loads[0].wait()
    loads[1].wait()
    factor_reds(blocks, factor, inverse, work, packed)
    for load in loads[2:]:
        load.wait()
    compact(
        lambda p, q: inverse[0, tile_rows(p), tile_rows(q)], order, mine, True
    )
    U, L, D, R = (slice(k * order, (k + 1) * order) for k in range(4))
    up_, left_, down_, right_ = (own.at[:, at] for at in (U, L, D, R))
    one = own_parts(packed, 1)
    solve(one, upright.at[1, 1], False, down_)
    inverse_up = remote(mine, inv_up, 5, (above, c))
    inverse_right = remote(mine, inv_right, 6, (r, left))
    left_up.append(remote(hor.at[0, 1, half:], from_up.at[2, half:], 10, (above, right)))
    compact_gram(down_, give_down)
    solve(one, flat.at[1, 1], False, right_)
    sent_down = remote(give_down, got_above, 7, (beneath, c))
    compact_gram(right_, give_sym)

    def give(rows, total):
        give_cross[rows, :] = total.astype(jnp.bfloat16)

    grams(order, [([(right_, down_)], give)])
    solve(one, upright.at[0, 1], True, up_)
    sent_sym = remote(give_sym, got_sym, 8, (r, right))
    sent_cross = remote(give_cross, got_cross, 9, (r, right))
    solve(one, flat.at[1, 0], True, left_)
    zero = own_parts(packed, 0)
    down, across = own_right.at[:, :order], own_right.at[:, order:]
    solve(zero, upright.at[0, 0], False, down)
    solve(zero, flat.at[0, 0], False, across)
    grams(
        order,
        [
            ([(across, across), (up_, up_)], subtract_into(schur.at[0])),
            ([(up_, down_)], negate_into(links.at[0, 1])),
            ([(across, down), (up_, left_)], negate_into(links.at[0, 3])),
            ([(down, down), (left_, left_)], subtract_into(schur.at[1])),
            ([(left_, right_)], negate_into(links.at[1, 0])),
        ],
    )
    down_right.wait_recv()
    right_right.wait_recv()
    inverse_right.wait_recv()
    near_left, near_down, near_right = (near.at[:, k * order : (k + 1) * order] for k in range(3))
    far = far_parts(inv_right, diag_right, order)
    solve(far, flat.at[0, 1], True, near_left)
    solve(far, from_right.at[0], False, near_down)
    solve(far, from_right.at[1], False, near_right)
    grams(
        order,
        [
            ([(near_left, near_left)], subtract_into(schur.at[0])),
            ([(near_left, near_right)], negate_into(links.at[0, 0])),
            ([(up_, right_), (near_left, near_down)], negate_into(links.at[0, 2])),
        ],
    )
    down_up.wait_recv()
    right_up.wait_recv()
    inverse_up.wait_recv()
    below_up, below_left, below_down, below_right = (near_up.at[:, at] for at in (U, L, D, R))
    far = far_parts(inv_up, diag_up, order)
    solve(far, upright.at[1, 0], True, below_up)
    solve(far, from_up.at[0], False, below_down)
    solve(far, from_up.at[1], False, below_right)
    grams(
        order,
        [
            ([(below_up, below_up)], subtract_into(schur.at[1])),
            ([(below_up, below_down)], negate_into(links.at[1, 1])),
            ([(left_, down_), (below_up, below_right)], negate_into(links.at[1, 2])),
        ],
    )
    sent_sym.wait_recv()
    subtract_compact(got_sym, schur.at[1])
    sent_cross.wait_recv()
    for k in range(2):
        part = slice(k * half, (k + 1) * half)
        left_up[k].wait_recv()
        solve(far, from_up.at[2, part], True, below_left.at[:, part])
        grams(
            order,
            [
                (
                    [(below_up, below_left.at[:, part])],
                    negate_with(got_cross.at[:, part], links.at[1, 3, :, part]),
                )
            ],
        )
    sent_down.wait_recv()
    subtract_compact(got_above, schur.at[0])
    for copy in (
        down_up, right_up, *left_up, down_right, right_right,
        inverse_up, inverse_right, sent_down, sent_sym, sent_cross,
    ):
        copy.wait_send()


def output_kernel(*refs):
    count = (len(refs) - 1) // 2
    copies = [
        pltpu.make_async_copy(refs[k], refs[count + k], refs[-1].at[k]) for k in range(count)
    ]
    for copy in copies:
        copy.start()
    for copy in copies:
        copy.wait()


def put_out(*arrays):
    return pl.pallas_call(
        output_kernel,
        out_shape=tuple(jax.ShapeDtypeStruct(a.shape, a.dtype) for a in arrays),
        in_specs=[VMEM] * len(arrays),
        out_specs=(HBM,) * len(arrays),
        scratch_shapes=[pltpu.SemaphoreType.DMA((len(arrays),))],
        compiler_params=pltpu.CompilerParams(vmem_limit_bytes=16 * 2**20),
    )(*arrays)


def on_device(diag_blocks, horizontal, vertical):
    order = diag_blocks.shape[-1]
    assert diag_blocks.shape[:2] == (2, 2)
    tiles = len(triangle(order))
    square = (order, order)
    bf16, f32 = jnp.bfloat16, jnp.float32
    dense = (compact_rows(order), PANEL)
    diagonal = (order // PANEL, PANEL, PANEL)
    outs = pl.pallas_call(
        whole_kernel,
        out_shape=(
            jax.ShapeDtypeStruct((2,) + square, f32),
            jax.ShapeDtypeStruct((2,) + square, f32),
            jax.ShapeDtypeStruct((2, 4) + square, bf16),
        ),
        in_specs=[HBM] * 3,
        out_specs=(VMEM, VMEM, VMEM),
        scratch_shapes=[
            pltpu.VMEM((2,) + square, f32),
            pltpu.VMEM((2,) + square, f32),
            pltpu.VMEM((2, PANEL, 2 * PANEL), f32),
            pltpu.VMEM((2, 2, tiles, PANEL, PANEL), bf16),
            pltpu.VMEM((2, 2) + square, bf16),
            pltpu.VMEM((2, 2) + square, bf16),
            pltpu.VMEM((3,) + square, bf16),
            pltpu.VMEM((2,) + square, bf16),
            pltpu.VMEM(dense, bf16),
            pltpu.VMEM(dense, bf16),
            pltpu.VMEM(dense, bf16),
            pltpu.VMEM(diagonal, bf16),
            pltpu.VMEM(diagonal, bf16),
            pltpu.VMEM((order, 4 * order), bf16),
            pltpu.VMEM((order, 2 * order), bf16),
            pltpu.VMEM((order, 3 * order), bf16),
            pltpu.VMEM((order, 4 * order), bf16),
            pltpu.VMEM(dense, bf16),
            pltpu.VMEM(dense, bf16),
            pltpu.VMEM(square, bf16),
            pltpu.VMEM(dense, bf16),
            pltpu.VMEM(square, bf16),
            pltpu.VMEM(dense, bf16),
            pltpu.SemaphoreType.DMA((6,)),
            pltpu.SemaphoreType.DMA((11,)),
            pltpu.SemaphoreType.DMA((11,)),
        ],
        compiler_params=pltpu.CompilerParams(
            collective_id=0, has_side_effects=True, vmem_limit_bytes=42 * 2**20
        ),
        cost_estimate=pl.CostEstimate(
            flops=20_000_000_000, bytes_accessed=8 * diag_blocks.size, transcendentals=0
        ),
    )(*(pltpu.with_memory_space_constraint(a, pltpu.HBM) for a in (diag_blocks, horizontal, vertical)))
    factor, schur, links = put_out(*outs)
    return (factor[:, None], schur[:, None], links[:, None])


def solution(mesh):
    in_specs = (
        P("row", "col", None, None),
        P("row", "col", None, None),
        P("row", "col", None, None),
    )
    out_specs = (
        P("row", "col", None, None),
        P("row", "col", None, None),
        P("row", "col", None, None, None),
    )
    return jax.shard_map(
        on_device, mesh=mesh, in_specs=in_specs, out_specs=out_specs, check_vma=False
    )
```

```python
import functools

import jax
import jax.numpy as jnp
from jax import lax
from jax.experimental import pallas as pl
from jax.experimental.pallas import tpu as pltpu
from jax.sharding import PartitionSpec as P


PANEL = 128
STRIP = 16
EIGHT = 8
HALF = 256
ROW_TILE = 16
VMEM = pl.BlockSpec(memory_space=pltpu.VMEM)
HBM = pl.BlockSpec(memory_space=pltpu.HBM)
TN = (((0,), (0,)), ((), ()))


def split(value):
    high = value.astype(jnp.bfloat16)
    low = (value - high.astype(jnp.float32)).astype(jnp.bfloat16)
    return high, low


def product(left, right):
    dot = functools.partial(jnp.dot, preferred_element_type=jnp.float32)
    (lh, ll), (rh, rl) = left, right
    return dot(lh, rh) + (dot(lh, rl) + dot(ll, rh))


def factor_diagonal(work, count):
    lane = lax.broadcasted_iota(jnp.int32, (EIGHT, PANEL), 1)
    sub = lax.broadcasted_iota(jnp.int32, (EIGHT, PANEL), 0)
    lane_tall = lax.broadcasted_iota(jnp.int32, (STRIP, PANEL), 1)
    groups = STRIP // EIGHT

    def spread(value, k):
        return jnp.broadcast_to(value[k : k + 1], value.shape)

    def strip(b, carry):
        start = pl.multiple_of(b * STRIP, STRIP)
        rows = [
            [
                [
                    work[m, pl.ds(pl.multiple_of(start + g * EIGHT, EIGHT), EIGHT), tile_rows(w)]
                    for w in range(2)
                ]
                for g in range(groups)
            ]
            for m in range(count)
        ]
        columns = [
            [
                [
                    jnp.take_along_axis(rows[m][g][0], jnp.full_like(lane, start + c), axis=1)
                    if g >= c // EIGHT
                    else None
                    for g in range(groups)
                ]
                for c in range(STRIP)
            ]
            for m in range(count)
        ]
        roots = [[jnp.zeros((EIGHT, PANEL), jnp.float32)] * groups for _ in range(count)]
        for j in range(STRIP):
            top, at = j // EIGHT, j % EIGHT
            for m in range(count):
                column = columns[m][j]
                root = lax.rsqrt(spread(column[top], at))
                square = root * root
                scaled = [None if v is None else v * square for v in column]
                for c in range(j + 1, STRIP):
                    across = spread(column[c // EIGHT], c % EIGHT)
                    for g in range(c // EIGHT, groups):
                        if c == j + 1:
                            term = (column[g] * across) * square
                        else:
                            term = scaled[g] * across
                        columns[m][c][g] = columns[m][c][g] - term
                roots[m][top] = jnp.where(sub == at, root, roots[m][top])
                line = [spread(v, at) for v in rows[m][top]]
                for g in range(top, groups):
                    below = scaled[g] if g > top else jnp.where(sub > at, scaled[g], 0.0)
                    rows[m][g] = [v - below * x for v, x in zip(rows[m][g], line)]
        for m in range(count):
            final = [
                jnp.concatenate([rows[m][g][w] * roots[m][g] for g in range(groups)], 0)
                for w in range(2)
            ]
            for w in range(2):
                work[m, pl.ds(start, STRIP), tile_rows(w)] = final[w]
            high = [v.astype(jnp.bfloat16).astype(jnp.float32) for v in final]
            low = [v - h for v, h in zip(final, high)]
            after = lane_tall >= start + STRIP
            left_high = jnp.where(after, high[0], 0.0)
            left_low = jnp.where(after, low[0], 0.0)
            left = jnp.concatenate([left_high, left_high, left_low, left_low], 0)
            wide_high, wide_low = jnp.concatenate(high, 1), jnp.concatenate(low, 1)
            right = jnp.concatenate([wide_high, wide_low, wide_high, wide_low], 0)
            work[m] = work[m] - lax.dot_general(
                left.astype(jnp.bfloat16).T,
                right.astype(jnp.bfloat16),
                (((1,), (0,)), ((), ())),
                preferred_element_type=jnp.float32,
            )
        return carry

    lax.fori_loop(0, PANEL // STRIP, strip, 0)


def triangle(order):
    return [(p, q) for p in range(order // PANEL) for q in range(p + 1)]


def factor_reds(blocks, factor, inverse, work, packed):
    count, order = blocks.shape[0], blocks.shape[2]
    row = lax.broadcasted_iota(jnp.int32, (PANEL, PANEL), 0)
    col = lax.broadcasted_iota(jnp.int32, (PANEL, PANEL), 1)
    eye = jnp.where(row == col, 1.0, 0.0).astype(jnp.float32)
    inverse[...] = jnp.zeros_like(inverse)
    factor[...] = jnp.zeros_like(factor)
    for start in range(0, order, PANEL):
        stop = start + PANEL
        here = slice(start, stop)
        for m in range(count):
            work[m, :, :PANEL] = blocks[m, here, here]
            work[m, :, PANEL:] = eye
        factor_diagonal(work, count)
        for m in range(count):
            upper = jnp.where(col >= row, work[m, :, :PANEL], 0.0)
            factor[m, here, here] = upper.T
            small = jnp.where(col <= row, work[m, :, PANEL:], 0.0)
            small_parts = split(small)
            if start:
                inverse[m, here, :start] = product(small_parts, split(inverse[m, here, :start]))
            inverse[m, here, here] = small
            if stop < order:
                across = product(small_parts, split(blocks[m, here, stop:]))
                down = across.T
                factor[m, stop:, here] = down
                down_parts = split(down)
                blocks[m, stop:, stop:] -= product(down_parts, split(across))
                inverse[m, stop:, :stop] -= product(down_parts, split(inverse[m, here, :stop]))
    for m in range(count):
        for n, (p, q) in enumerate(triangle(order)):
            tile = inverse[m, p * PANEL : (p + 1) * PANEL, q * PANEL : (q + 1) * PANEL]
            packed[m, 0, n], packed[m, 1, n] = split(tile)


def triangle_index(p, q):
    return p * (p + 1) // 2 + q


def off_diagonal(order):
    return [(p, q) for p, q in triangle(order) if p != q]


def grid_of_panel():
    row = lax.broadcasted_iota(jnp.int32, (PANEL, PANEL), 0)
    col = lax.broadcasted_iota(jnp.int32, (PANEL, PANEL), 1)
    return row, col


def compact_rows(order):
    panels = order // PANEL
    return (len(off_diagonal(order)) + panels // 2) * PANEL + ROW_TILE


def tile_rows(n):
    return slice(n * PANEL, (n + 1) * PANEL)


def compact(tile_of, order, out, flip):
    row, col = grid_of_panel()
    pairs = off_diagonal(order)
    for n, (p, q) in enumerate(pairs):
        out[tile_rows(n), :] = tile_of(p, q).astype(jnp.bfloat16)
    lines = []
    for k in range(0, order // PANEL, 2):
        first, second = tile_of(k, k), tile_of(k + 1, k + 1)
        other = second.T if flip else second
        joined = jnp.where(row >= col, first, other)
        out[tile_rows(len(pairs) + k // 2), :] = joined.astype(jnp.bfloat16)
        lines.append(jnp.sum(jnp.where(row == col, second, 0.0), axis=0, keepdims=True))
    lines.append(jnp.zeros((ROW_TILE - len(lines), PANEL), jnp.float32))
    base = compact_rows(order) - ROW_TILE
    out[base:, :] = jnp.concatenate(lines, 0).astype(jnp.bfloat16)


def spread_diagonal(packed, order, symmetric):
    row, col = grid_of_panel()
    skip = len(off_diagonal(order))
    base = compact_rows(order) - ROW_TILE
    lines = packed[base:, :].astype(jnp.float32)
    tiles = []
    for k in range(order // PANEL // 2):
        joined = packed[tile_rows(skip + k), :].astype(jnp.float32)
        turned = joined.T
        line = jnp.broadcast_to(lines[k : k + 1, :], joined.shape)
        tiles.append(jnp.where(row >= col, joined, turned if symmetric else 0.0))
        upper = joined if symmetric else 0.0
        tiles.append(jnp.where(row == col, line, jnp.where(col < row, turned, upper)))
    return tiles


def solve(parts, coupling, flipped, out):
    order = out.shape[0]
    axes = (((1,), (1 if flipped else 0,)), ((), ()))
    zero = jnp.zeros((PANEL, PANEL), jnp.bfloat16)
    for top in range(0, order // PANEL, 2):
        stop = (top + 2) * PANEL
        right = coupling[:, :stop] if flipped else coupling[:stop, :]
        value = None
        for tile_of in parts:
            lines = [
                jnp.concatenate([tile_of(p, q) if q <= p else zero for q in range(top + 2)], 1)
                for p in (top, top + 1)
            ]
            left = jnp.concatenate(lines, 0)
            term = lax.dot_general(left, right, axes, preferred_element_type=jnp.float32)
            value = term if value is None else value + term
        out[top * PANEL : stop, :] = value.astype(jnp.bfloat16)


def own_parts(packed, m):
    return [
        lambda p, q, part=part: packed[m, part, triangle_index(p, q)] for part in range(2)
    ]


def far_parts(packed, diagonal, order):
    for k, tile in enumerate(spread_diagonal(packed, order, False)):
        diagonal[k] = tile.astype(jnp.bfloat16)
    place = {pair: n for n, pair in enumerate(off_diagonal(order))}
    return [lambda p, q: diagonal[p] if p == q else packed[tile_rows(place[p, q]), :]]


def grams(order, terms):
    def body(step, carry):
        rows = pl.ds(pl.multiple_of(step * HALF, HALF), HALF)
        for pairs, emit in terms:
            total = None
            for left, right in pairs:
                value = lax.dot_general(
                    left[:, rows], right[...], TN, preferred_element_type=jnp.float32
                )
                total = value if total is None else total + value
            emit(rows, total)
        return carry

    lax.fori_loop(0, order // HALF, body, 0)


def compact_gram(solved, out):
    order = solved.shape[0]
    strips = [
        lax.dot_general(
            solved[:, tile_rows(p)],
            solved[:, : (p + 1) * PANEL],
            TN,
            preferred_element_type=jnp.float32,
        )
        for p in range(order // PANEL)
    ]
    compact(lambda p, q: strips[p][:, tile_rows(q)], order, out, False)


def difference_into(start, out):
    def emit(rows, total):
        out[rows, :] = start[rows, :] - total

    return emit


def negate_into(out):
    def emit(rows, total):
        out[rows, :] = (-total).astype(jnp.bfloat16)

    return emit


def negate_with(extra, out):
    def emit(rows, total):
        out[rows, :] = (-(total + extra[rows, :].astype(jnp.float32))).astype(jnp.bfloat16)

    return emit


def plain_into(out):
    def emit(rows, total):
        out[rows, :] = total.astype(jnp.bfloat16)

    return emit


class Mover:
    def __init__(self, sems):
        self.sems, self.copies = sems, []

    def start(self, src, dst):
        copy = pltpu.make_async_copy(src, dst, self.sems.at[len(self.copies)])
        copy.start()
        self.copies.append([copy, False])
        return len(self.copies) - 1

    def wait(self, *which):
        for k in which or range(len(self.copies)):
            copy, done = self.copies[k]
            if not done:
                copy.wait()
                self.copies[k][1] = True


def factor_kernel(
    diag, hor, ver,
    factor_out, packed, mine, down, give_down, flat, upright, start,
    blocks, factor, inverse, work, sems,
):
    order = blocks.shape[1]
    mover = Mover(sems)
    for m in range(2):
        mover.start(diag.at[m, m], blocks.at[m])
    mover.wait()
    mover.start(ver, upright)
    mover.start(hor, flat)
    mover.start(diag.at[0, 1], start.at[0])
    mover.start(diag.at[1, 0], start.at[1])
    factor_reds(blocks, factor, inverse, work, packed)
    out = mover.start(factor, factor_out)
    compact(lambda p, q: inverse[0, tile_rows(p), tile_rows(q)], order, mine, True)
    mover.wait(*range(2, out))
    solve(own_parts(packed, 1), upright.at[1, 1], False, down)
    compact_gram(down, give_down)
    mover.wait(out)


def give_kernel(packed, down, flat, right, give_sym, give_cross):
    order = right.shape[0]
    solve(own_parts(packed, 1), flat.at[1, 1], False, right)
    compact_gram(right, give_sym)
    grams(order, [([(right, down)], plain_into(give_cross))])


def own_kernel(
    packed, down_, right_, start, flat, upright,
    schur0, schur1, up_, left_, made,
    own,
):
    order = up_.shape[0]
    one, zero = own_parts(packed, 1), own_parts(packed, 0)
    down, across = own.at[0], own.at[1]
    solve(one, flat.at[1, 0], True, left_)
    solve(one, upright.at[0, 1], True, up_)
    solve(zero, upright.at[0, 0], False, down)
    solve(zero, flat.at[0, 0], False, across)
    grams(
        order,
        [
            ([(across, across), (up_, up_)], difference_into(start.at[0], schur0)),
            ([(down, down), (left_, left_)], difference_into(start.at[1], schur1)),
            ([(up_, down_)], negate_into(made.at[0])),
            ([(across, down), (up_, left_)], negate_into(made.at[1])),
            ([(left_, right_)], negate_into(made.at[2])),
        ],
    )


def right_kernel(
    inv, far_down, far_right, flat, schur_in, up_, right_, ready,
    schur, made, links_out,
    diagonal, near, sems,
):
    order = up_.shape[0]
    mover = Mover(sems)
    mover.start(ready.at[0], links_out.at[0, 0, 1])
    mover.start(ready.at[1], links_out.at[0, 0, 3])
    mover.start(ready.at[2], links_out.at[1, 0, 0])
    far = far_parts(inv, diagonal, order)
    near_left, near_down, near_right = near.at[0], near.at[1], near.at[2]
    solve(far, flat.at[0, 1], True, near_left)
    solve(far, far_down, False, near_down)
    solve(far, far_right, False, near_right)
    grams(
        order,
        [
            ([(near_left, near_left)], difference_into(schur_in, schur)),
            ([(near_left, near_right)], negate_into(made.at[0])),
            ([(up_, right_), (near_left, near_down)], negate_into(made.at[1])),
        ],
    )
    mover.wait()


def below_kernel(
    inv, far_down, far_right, far_left, upright, schur_in, down_, left_, got_cross,
    ready, links_in,
    schur, links_out,
    diagonal, near, made, sems,
):
    order = down_.shape[0]
    mover = Mover(sems)
    mover.start(ready.at[0], links_out.at[0, 0, 0])
    mover.start(ready.at[1], links_out.at[0, 0, 2])
    far = far_parts(inv, diagonal, order)
    below_up, below_left, below_down, below_right = (near.at[k] for k in range(4))
    solve(far, upright.at[1, 0], True, below_up)
    solve(far, far_down, False, below_down)
    solve(far, far_right, False, below_right)
    solve(far, far_left, True, below_left)
    grams(
        order,
        [
            ([(below_up, below_up)], difference_into(schur_in, schur)),
            ([(below_up, below_down)], negate_into(made.at[0])),
            ([(left_, down_), (below_up, below_right)], negate_into(made.at[1])),
        ],
    )
    mover.start(made.at[0], links_out.at[1, 0, 1])
    mover.start(made.at[1], links_out.at[1, 0, 2])
    grams(order, [([(below_up, below_left)], negate_with(got_cross, made.at[2]))])
    mover.start(made.at[2], links_out.at[1, 0, 3])
    mover.wait()


def subtracted(packed, whole, out, mover, place):
    order = out.shape[0]
    panels = order // PANEL
    spread = spread_diagonal(packed, order, True)
    index = {pair: n for n, pair in enumerate(off_diagonal(order))}
    tiles = {pair: packed[tile_rows(n), :].astype(jnp.float32) for pair, n in index.items()}
    for p in range(panels):
        line = [
            spread[p] if q == p else tiles[p, q] if q < p else tiles[q, p].T
            for q in range(panels)
        ]
        out[tile_rows(p), :] = whole[tile_rows(p), :] - jnp.concatenate(line, 1)
        mover.start(out.at[tile_rows(p)], place.at[tile_rows(p)])


def schur_odd_kernel(partial, got, schur_out, schur, sems):
    mover = Mover(sems)
    subtracted(got, partial, schur, mover, schur_out.at[1, 0])
    mover.wait()


def schur_even_kernel(partial, got, schur_in, schur_out, schur, sems):
    mover = Mover(sems)
    subtracted(got, partial, schur, mover, schur_out.at[0, 0])
    mover.wait()


def first_kernel(hor, ver, down, right, left, sems):
    mover = Mover(sems)
    mover.start(ver.at[0, 0], down)
    mover.start(hor.at[0, 0], right)
    mover.start(hor.at[0, 1], left)
    mover.wait()


def called(kernel, ins, outs, scratch, flops, aliases=None):
    size = sum(a.size * a.dtype.itemsize for a, _ in ins)
    held = [
        pltpu.with_memory_space_constraint(a, pltpu.HBM) if spec is HBM else a for a, spec in ins
    ]
    return pl.pallas_call(
        kernel,
        out_shape=tuple(jax.ShapeDtypeStruct(shape, dtype) for shape, dtype, _ in outs),
        in_specs=[spec for _, spec in ins],
        out_specs=tuple(spec for _, _, spec in outs),
        scratch_shapes=scratch,
        input_output_aliases=aliases or {},
        compiler_params=pltpu.CompilerParams(vmem_limit_bytes=24 * 2**20),
        cost_estimate=pl.CostEstimate(flops=flops, bytes_accessed=size, transcendentals=0),
    )(*held)


def shifted(value, down, across):
    rows, cols = lax.axis_size("row"), lax.axis_size("col")
    pairs = [
        (i * cols + j, (i + down) % rows * cols + (j + across) % cols)
        for i in range(rows)
        for j in range(cols)
    ]
    return lax.ppermute(value, ("row", "col"), pairs)


def on_device(diag_blocks, horizontal, vertical):
    order = diag_blocks.shape[-1]
    assert diag_blocks.shape[:2] == (2, 2)
    tiles = len(triangle(order))
    square = (order, order)
    bf16, f32 = jnp.bfloat16, jnp.float32
    dense = (compact_rows(order), PANEL)
    diagonal = pltpu.VMEM((order // PANEL, PANEL, PANEL), bf16)

    def sems(n):
        return pltpu.SemaphoreType.DMA((n,))

    down_first, right_first, left_first = called(
        first_kernel,
        [(horizontal, HBM), (vertical, HBM)],
        [(square, bf16, VMEM)] * 3,
        [sems(3)],
        1_000_000,
    )
    down_up = shifted(down_first, -1, 0)
    right_up = shifted(right_first, -1, 0)
    left_up = shifted(left_first, -1, 1)
    down_right = shifted(down_first, 0, -1)
    right_right = shifted(right_first, 0, -1)
    pairs = (2, 2) + square
    factor, packed, mine, down, give_down, flat, upright, start = called(
        factor_kernel,
        [(diag_blocks, HBM), (horizontal, HBM), (vertical, HBM)],
        [
            ((2,) + square, f32, HBM),
            ((2, 2, tiles, PANEL, PANEL), bf16, VMEM),
            (dense, bf16, VMEM),
            (square, bf16, VMEM),
            (dense, bf16, VMEM),
            (pairs, bf16, VMEM),
            (pairs, bf16, VMEM),
            ((2,) + square, f32, VMEM),
        ],
        [
            pltpu.VMEM((2,) + square, f32),
            pltpu.VMEM((2,) + square, f32),
            pltpu.VMEM((2,) + square, f32),
            pltpu.VMEM((2, PANEL, 2 * PANEL), f32),
            sems(7),
        ],
        20_000_000_000,
    )
    inverse_up = shifted(mine, -1, 0)
    inverse_right = shifted(mine, 0, -1)
    got_above = shifted(give_down, 1, 0)
    right, give_sym, give_cross = called(
        give_kernel,
        [(packed, VMEM), (down, VMEM), (flat, VMEM)],
        [(square, bf16, VMEM), (dense, bf16, VMEM), (square, bf16, VMEM)],
        [],
        1_000_000_000,
    )
    got_sym = shifted(give_sym, 0, 1)
    got_cross = shifted(give_cross, 0, 1)
    links_shape = ((2, 1, 4) + square, bf16, HBM)
    schur0, schur1, up, left, ready = called(
        own_kernel,
        [(packed, VMEM), (down, VMEM), (right, VMEM), (start, VMEM), (flat, VMEM), (upright, VMEM)],
        [
            (square, f32, VMEM), (square, f32, VMEM),
            (square, bf16, VMEM), (square, bf16, VMEM), ((3,) + square, bf16, VMEM),
        ],
        [pltpu.VMEM((2,) + square, bf16)],
        3_000_000_000,
    )
    schur0, ready, links = called(
        right_kernel,
        [
            (inverse_right, VMEM), (down_right, VMEM), (right_right, VMEM), (flat, VMEM),
            (schur0, VMEM), (up, VMEM), (right, VMEM), (ready, VMEM),
        ],
        [(square, f32, VMEM), ((2,) + square, bf16, VMEM), links_shape],
        [diagonal, pltpu.VMEM((3,) + square, bf16), sems(3)],
        2_000_000_000,
    )
    schur1, links = called(
        below_kernel,
        [
            (inverse_up, VMEM), (down_up, VMEM), (right_up, VMEM), (left_up, VMEM),
            (upright, VMEM), (schur1, VMEM), (down, VMEM), (left, VMEM),
            (got_cross, VMEM), (ready, VMEM), (links, HBM),
        ],
        [(square, f32, VMEM), links_shape],
        [
            diagonal, pltpu.VMEM((4,) + square, bf16), pltpu.VMEM((3,) + square, bf16), sems(5),
        ],
        3_000_000_000,
        {10: 1},
    )
    schur_shape = ((2, 1) + square, f32, HBM)
    strips = sems(order // PANEL)
    (schur,) = called(
        schur_odd_kernel,
        [(schur1, VMEM), (got_sym, VMEM)],
        [schur_shape],
        [pltpu.VMEM(square, f32), strips],
        300_000_000,
    )
    (schur,) = called(
        schur_even_kernel,
        [(schur0, VMEM), (got_above, VMEM), (schur, HBM)],
        [schur_shape],
        [pltpu.VMEM(square, f32), strips],
        300_000_000,
        {2: 0},
    )
    return (factor[:, None], schur, links)


def solution(mesh):
    in_specs = (
        P("row", "col", None, None),
        P("row", "col", None, None),
        P("row", "col", None, None),
    )
    out_specs = (
        P("row", "col", None, None),
        P("row", "col", None, None),
        P("row", "col", None, None, None),
    )
    return jax.shard_map(
        on_device, mesh=mesh, in_specs=in_specs, out_specs=out_specs, check_vma=False
    )
```

```python
import functools

import jax
import jax.numpy as jnp
from jax import lax
from jax.experimental import pallas as pl
from jax.experimental.pallas import tpu as pltpu
from jax.sharding import PartitionSpec as P


PANEL = 128
STRIP = 16
EIGHT = 8
HALF = 256
ROW_TILE = 16
VMEM = pl.BlockSpec(memory_space=pltpu.VMEM)
HBM = pl.BlockSpec(memory_space=pltpu.HBM)
TN = (((0,), (0,)), ((), ()))


def split(value):
    high = value.astype(jnp.bfloat16)
    low = (value - high.astype(jnp.float32)).astype(jnp.bfloat16)
    return high, low


def product(left, right):
    dot = functools.partial(jnp.dot, preferred_element_type=jnp.float32)
    (lh, ll), (rh, rl) = left, right
    return dot(lh, rh) + (dot(lh, rl) + dot(ll, rh))


def factor_diagonal(work, count):
    lane = lax.broadcasted_iota(jnp.int32, (EIGHT, PANEL), 1)
    sub = lax.broadcasted_iota(jnp.int32, (EIGHT, PANEL), 0)
    lane_tall = lax.broadcasted_iota(jnp.int32, (STRIP, PANEL), 1)
    groups = STRIP // EIGHT

    def spread(value, k):
        return jnp.broadcast_to(value[k : k + 1], value.shape)

    def strip(b, carry):
        start = pl.multiple_of(b * STRIP, STRIP)
        rows = [
            [
                [
                    work[m, pl.ds(pl.multiple_of(start + g * EIGHT, EIGHT), EIGHT), tile_rows(w)]
                    for w in range(2)
                ]
                for g in range(groups)
            ]
            for m in range(count)
        ]
        columns = [
            [
                [
                    jnp.take_along_axis(rows[m][g][0], jnp.full_like(lane, start + c), axis=1)
                    if g >= c // EIGHT
                    else None
                    for g in range(groups)
                ]
                for c in range(STRIP)
            ]
            for m in range(count)
        ]
        roots = [[jnp.zeros((EIGHT, PANEL), jnp.float32)] * groups for _ in range(count)]
        for j in range(STRIP):
            top, at = j // EIGHT, j % EIGHT
            for m in range(count):
                column = columns[m][j]
                root = lax.rsqrt(spread(column[top], at))
                square = root * root
                scaled = [None if v is None else v * square for v in column]
                for c in range(j + 1, STRIP):
                    across = spread(column[c // EIGHT], c % EIGHT)
                    for g in range(c // EIGHT, groups):
                        if c == j + 1:
                            term = (column[g] * across) * square
                        else:
                            term = scaled[g] * across
                        columns[m][c][g] = columns[m][c][g] - term
                roots[m][top] = jnp.where(sub == at, root, roots[m][top])
                line = [spread(v, at) for v in rows[m][top]]
                for g in range(top, groups):
                    below = scaled[g] if g > top else jnp.where(sub > at, scaled[g], 0.0)
                    rows[m][g] = [v - below * x for v, x in zip(rows[m][g], line)]
        for m in range(count):
            final = [
                jnp.concatenate([rows[m][g][w] * roots[m][g] for g in range(groups)], 0)
                for w in range(2)
            ]
            for w in range(2):
                work[m, pl.ds(start, STRIP), tile_rows(w)] = final[w]
            high = [v.astype(jnp.bfloat16).astype(jnp.float32) for v in final]
            low = [v - h for v, h in zip(final, high)]
            after = lane_tall >= start + STRIP
            left_high = jnp.where(after, high[0], 0.0)
            left_low = jnp.where(after, low[0], 0.0)
            left = jnp.concatenate([left_high, left_high, left_low, left_low], 0)
            wide_high, wide_low = jnp.concatenate(high, 1), jnp.concatenate(low, 1)
            right = jnp.concatenate([wide_high, wide_low, wide_high, wide_low], 0)
            work[m] = work[m] - lax.dot_general(
                left.astype(jnp.bfloat16).T,
                right.astype(jnp.bfloat16),
                (((1,), (0,)), ((), ())),
                preferred_element_type=jnp.float32,
            )
        return carry

    lax.fori_loop(0, PANEL // STRIP, strip, 0)


def triangle(order):
    return [(p, q) for p in range(order // PANEL) for q in range(p + 1)]


def factor_reds(blocks, factor, inverse, work, packed):
    count, order = blocks.shape[0], blocks.shape[2]
    row = lax.broadcasted_iota(jnp.int32, (PANEL, PANEL), 0)
    col = lax.broadcasted_iota(jnp.int32, (PANEL, PANEL), 1)
    eye = jnp.where(row == col, 1.0, 0.0).astype(jnp.float32)
    inverse[...] = jnp.zeros_like(inverse)
    factor[...] = jnp.zeros_like(factor)
    for start in range(0, order, PANEL):
        stop = start + PANEL
        here = slice(start, stop)
        for m in range(count):
            work[m, :, :PANEL] = blocks[m, here, here]
            work[m, :, PANEL:] = eye
        factor_diagonal(work, count)
        for m in range(count):
            upper = jnp.where(col >= row, work[m, :, :PANEL], 0.0)
            factor[m, here, here] = upper.T
            small = jnp.where(col <= row, work[m, :, PANEL:], 0.0)
            small_parts = split(small)
            if start:
                inverse[m, here, :start] = product(small_parts, split(inverse[m, here, :start]))
            inverse[m, here, here] = small
            if stop < order:
                across = product(small_parts, split(blocks[m, here, stop:]))
                down = across.T
                factor[m, stop:, here] = down
                down_parts = split(down)
                blocks[m, stop:, stop:] -= product(down_parts, split(across))
                inverse[m, stop:, :stop] -= product(down_parts, split(inverse[m, here, :stop]))
    for m in range(count):
        for n, (p, q) in enumerate(triangle(order)):
            tile = inverse[m, p * PANEL : (p + 1) * PANEL, q * PANEL : (q + 1) * PANEL]
            packed[m, 0, n], packed[m, 1, n] = split(tile)


def triangle_index(p, q):
    return p * (p + 1) // 2 + q


def off_diagonal(order):
    return [(p, q) for p, q in triangle(order) if p != q]


def grid_of_panel():
    row = lax.broadcasted_iota(jnp.int32, (PANEL, PANEL), 0)
    col = lax.broadcasted_iota(jnp.int32, (PANEL, PANEL), 1)
    return row, col


def compact_rows(order):
    panels = order // PANEL
    return (len(off_diagonal(order)) + panels // 2) * PANEL + ROW_TILE


def tile_rows(n):
    return slice(n * PANEL, (n + 1) * PANEL)


def compact(tile_of, order, out, flip):
    row, col = grid_of_panel()
    pairs = off_diagonal(order)
    for n, (p, q) in enumerate(pairs):
        out[tile_rows(n), :] = tile_of(p, q).astype(jnp.bfloat16)
    lines = []
    for k in range(0, order // PANEL, 2):
        first, second = tile_of(k, k), tile_of(k + 1, k + 1)
        other = second.T if flip else second
        joined = jnp.where(row >= col, first, other)
        out[tile_rows(len(pairs) + k // 2), :] = joined.astype(jnp.bfloat16)
        lines.append(jnp.sum(jnp.where(row == col, second, 0.0), axis=0, keepdims=True))
    lines.append(jnp.zeros((ROW_TILE - len(lines), PANEL), jnp.float32))
    base = compact_rows(order) - ROW_TILE
    out[base:, :] = jnp.concatenate(lines, 0).astype(jnp.bfloat16)


def spread_diagonal(packed, order, symmetric):
    row, col = grid_of_panel()
    skip = len(off_diagonal(order))
    base = compact_rows(order) - ROW_TILE
    lines = packed[base:, :].astype(jnp.float32)
    tiles = []
    for k in range(order // PANEL // 2):
        joined = packed[tile_rows(skip + k), :].astype(jnp.float32)
        turned = joined.T
        line = jnp.broadcast_to(lines[k : k + 1, :], joined.shape)
        tiles.append(jnp.where(row >= col, joined, turned if symmetric else 0.0))
        upper = joined if symmetric else 0.0
        tiles.append(jnp.where(row == col, line, jnp.where(col < row, turned, upper)))
    return tiles


def solve(parts, coupling, flipped, out):
    order = out.shape[0]
    axes = (((1,), (1 if flipped else 0,)), ((), ()))
    zero = jnp.zeros((PANEL, PANEL), jnp.bfloat16)
    for top in range(0, order // PANEL, 2):
        stop = (top + 2) * PANEL
        right = coupling[:, :stop] if flipped else coupling[:stop, :]
        value = None
        for tile_of in parts:
            lines = [
                jnp.concatenate([tile_of(p, q) if q <= p else zero for q in range(top + 2)], 1)
                for p in (top, top + 1)
            ]
            left = jnp.concatenate(lines, 0)
            term = lax.dot_general(left, right, axes, preferred_element_type=jnp.float32)
            value = term if value is None else value + term
        out[top * PANEL : stop, :] = value.astype(jnp.bfloat16)


def own_parts(packed, m):
    return [
        lambda p, q, part=part: packed[m, part, triangle_index(p, q)] for part in range(2)
    ]


def far_parts(packed, diagonal, order):
    for k, tile in enumerate(spread_diagonal(packed, order, False)):
        diagonal[k] = tile.astype(jnp.bfloat16)
    place = {pair: n for n, pair in enumerate(off_diagonal(order))}
    return [lambda p, q: diagonal[p] if p == q else packed[tile_rows(place[p, q]), :]]


def grams(order, terms):
    def body(step, carry):
        rows = pl.ds(pl.multiple_of(step * HALF, HALF), HALF)
        for pairs, emit in terms:
            total = None
            for left, right in pairs:
                value = lax.dot_general(
                    left[:, rows], right[...], TN, preferred_element_type=jnp.float32
                )
                total = value if total is None else total + value
            emit(rows, total)
        return carry

    lax.fori_loop(0, order // HALF, body, 0)


def compact_gram(solved, out):
    order = solved.shape[0]
    strips = [
        lax.dot_general(
            solved[:, tile_rows(p)],
            solved[:, : (p + 1) * PANEL],
            TN,
            preferred_element_type=jnp.float32,
        )
        for p in range(order // PANEL)
    ]
    compact(lambda p, q: strips[p][:, tile_rows(q)], order, out, False)


def difference_into(start, out):
    def emit(rows, total):
        out[rows, :] = start[rows, :] - total

    return emit


def negate_into(out):
    def emit(rows, total):
        out[rows, :] = (-total).astype(jnp.bfloat16)

    return emit


def negate_with(extra, out):
    def emit(rows, total):
        out[rows, :] = (-(total + extra[rows, :].astype(jnp.float32))).astype(jnp.bfloat16)

    return emit


def plain_into(out):
    def emit(rows, total):
        out[rows, :] = total.astype(jnp.bfloat16)

    return emit


class Mover:
    def __init__(self, sems):
        self.sems, self.copies = sems, []

    def start(self, src, dst):
        copy = pltpu.make_async_copy(src, dst, self.sems.at[len(self.copies)])
        copy.start()
        self.copies.append([copy, False])
        return len(self.copies) - 1

    def wait(self, *which):
        for k in which or range(len(self.copies)):
            copy, done = self.copies[k]
            if not done:
                copy.wait()
                self.copies[k][1] = True


def factor_kernel(
    diag, hor, ver,
    factor_out, packed, mine, down, give_down, flat, upright, start,
    blocks, factor, inverse, work, sems,
):
    order = blocks.shape[1]
    mover = Mover(sems)
    for m in range(2):
        mover.start(diag.at[m, m], blocks.at[m])
    mover.wait()
    mover.start(ver, upright)
    mover.start(hor, flat)
    mover.start(diag.at[0, 1], start.at[0])
    mover.start(diag.at[1, 0], start.at[1])
    factor_reds(blocks, factor, inverse, work, packed)
    out = mover.start(factor, factor_out)
    compact(lambda p, q: inverse[0, tile_rows(p), tile_rows(q)], order, mine, True)
    mover.wait(*range(2, out))
    solve(own_parts(packed, 1), upright.at[1, 1], False, down)
    compact_gram(down, give_down)
    mover.wait(out)


def give_kernel(packed, down, flat, right, give_sym, give_cross):
    order = right.shape[0]
    solve(own_parts(packed, 1), flat.at[1, 1], False, right)
    compact_gram(right, give_sym)
    grams(order, [([(right, down)], plain_into(give_cross))])


def own_kernel(
    packed, down_, right_, start, flat, upright,
    schur0, schur1, up_, left_, made,
    own,
):
    order = up_.shape[0]
    one, zero = own_parts(packed, 1), own_parts(packed, 0)
    down, across = own.at[0], own.at[1]
    solve(one, flat.at[1, 0], True, left_)
    solve(one, upright.at[0, 1], True, up_)
    solve(zero, upright.at[0, 0], False, down)
    solve(zero, flat.at[0, 0], False, across)
    grams(
        order,
        [
            ([(across, across), (up_, up_)], difference_into(start.at[0], schur0)),
            ([(down, down), (left_, left_)], difference_into(start.at[1], schur1)),
            ([(up_, down_)], negate_into(made.at[0])),
            ([(across, down), (up_, left_)], negate_into(made.at[1])),
            ([(left_, right_)], negate_into(made.at[2])),
        ],
    )


def right_kernel(
    inv, far_down, far_right, flat, schur_in, up_, right_, ready,
    schur, made, links_out,
    diagonal, near, sems,
):
    order = up_.shape[0]
    mover = Mover(sems)
    mover.start(ready.at[0], links_out.at[0, 0, 1])
    mover.start(ready.at[1], links_out.at[0, 0, 3])
    mover.start(ready.at[2], links_out.at[1, 0, 0])
    far = far_parts(inv, diagonal, order)
    near_left, near_down, near_right = near.at[0], near.at[1], near.at[2]
    solve(far, flat.at[0, 1], True, near_left)
    solve(far, far_down, False, near_down)
    solve(far, far_right, False, near_right)
    grams(
        order,
        [
            ([(near_left, near_left)], difference_into(schur_in, schur)),
            ([(near_left, near_right)], negate_into(made.at[0])),
            ([(up_, right_), (near_left, near_down)], negate_into(made.at[1])),
        ],
    )
    mover.wait()


def below_kernel(
    inv, far_down, far_right, far_left, upright, schur_in, down_, left_, got_cross,
    ready, links_in,
    schur, made, links_out,
    diagonal, near, sems,
):
    order = down_.shape[0]
    mover = Mover(sems)
    mover.start(ready.at[0], links_out.at[0, 0, 0])
    mover.start(ready.at[1], links_out.at[0, 0, 2])
    far = far_parts(inv, diagonal, order)
    below_up, below_left, below_down, below_right = (near.at[k] for k in range(4))
    solve(far, upright.at[1, 0], True, below_up)
    solve(far, far_down, False, below_down)
    solve(far, far_right, False, below_right)
    solve(far, far_left, True, below_left)
    grams(
        order,
        [
            ([(below_up, below_up)], difference_into(schur_in, schur)),
            ([(below_up, below_down)], negate_into(made.at[0])),
            ([(left_, down_), (below_up, below_right)], negate_into(made.at[1])),
        ],
    )
    grams(order, [([(below_up, below_left)], negate_with(got_cross, made.at[2]))])
    mover.wait()


def subtracted(packed, whole, out, mover, place):
    order = out.shape[0]
    panels = order // PANEL
    spread = spread_diagonal(packed, order, True)
    index = {pair: n for n, pair in enumerate(off_diagonal(order))}
    tiles = {pair: packed[tile_rows(n), :].astype(jnp.float32) for pair, n in index.items()}
    for p in reversed(range(panels)):
        line = [
            spread[p] if q == p else tiles[p, q] if q < p else tiles[q, p].T
            for q in range(panels)
        ]
        out[tile_rows(p), :] = whole[tile_rows(p), :] - jnp.concatenate(line, 1)
        mover.start(out.at[tile_rows(p)], place.at[tile_rows(p)])


def schur_odd_kernel(partial, got, ready, links_in, schur_out, links_out, schur, sems):
    mover = Mover(sems)
    for k in range(3):
        mover.start(ready.at[k], links_out.at[1, 0, 1 + k])
    subtracted(got, partial, schur, mover, schur_out.at[1, 0])
    mover.wait()


def schur_even_kernel(partial, got, schur_in, schur_out, schur, sems):
    mover = Mover(sems)
    subtracted(got, partial, schur, mover, schur_out.at[0, 0])
    mover.wait()


def left_kernel(hor, left, sems):
    mover = Mover(sems)
    mover.start(hor.at[0, 1], left)
    mover.wait()


def first_kernel(hor, ver, down, right, sems):
    mover = Mover(sems)
    mover.start(ver.at[0, 0], down)
    mover.start(hor.at[0, 0], right)
    mover.wait()


def called(kernel, ins, outs, scratch, flops, aliases=None):
    size = sum(a.size * a.dtype.itemsize for a, _ in ins)
    held = [
        pltpu.with_memory_space_constraint(a, pltpu.HBM) if spec is HBM else a for a, spec in ins
    ]
    return pl.pallas_call(
        kernel,
        out_shape=tuple(jax.ShapeDtypeStruct(shape, dtype) for shape, dtype, _ in outs),
        in_specs=[spec for _, spec in ins],
        out_specs=tuple(spec for _, _, spec in outs),
        scratch_shapes=scratch,
        input_output_aliases=aliases or {},
        compiler_params=pltpu.CompilerParams(vmem_limit_bytes=24 * 2**20),
        cost_estimate=pl.CostEstimate(flops=flops, bytes_accessed=size, transcendentals=0),
    )(*held)


def shifted(value, down, across):
    rows, cols = lax.axis_size("row"), lax.axis_size("col")
    pairs = [
        (i * cols + j, (i + down) % rows * cols + (j + across) % cols)
        for i in range(rows)
        for j in range(cols)
    ]
    return lax.ppermute(value, ("row", "col"), pairs)


def on_device(diag_blocks, horizontal, vertical):
    order = diag_blocks.shape[-1]
    assert diag_blocks.shape[:2] == (2, 2)
    tiles = len(triangle(order))
    square = (order, order)
    bf16, f32 = jnp.bfloat16, jnp.float32
    dense = (compact_rows(order), PANEL)
    diagonal = pltpu.VMEM((order // PANEL, PANEL, PANEL), bf16)

    def sems(n):
        return pltpu.SemaphoreType.DMA((n,))

    (left_first,) = called(
        left_kernel, [(horizontal, HBM)], [(square, bf16, VMEM)], [sems(1)], 1_000_000
    )
    left_up = shifted(left_first, -1, 1)
    down_first, right_first = called(
        first_kernel,
        [(horizontal, HBM), (vertical, HBM)],
        [(square, bf16, VMEM)] * 2,
        [sems(2)],
        1_000_000,
    )
    down_up = shifted(down_first, -1, 0)
    right_up = shifted(right_first, -1, 0)
    down_right = shifted(down_first, 0, -1)
    right_right = shifted(right_first, 0, -1)
    pairs = (2, 2) + square
    factor, packed, mine, down, give_down, flat, upright, start = called(
        factor_kernel,
        [(diag_blocks, HBM), (horizontal, HBM), (vertical, HBM)],
        [
            ((2,) + square, f32, HBM),
            ((2, 2, tiles, PANEL, PANEL), bf16, VMEM),
            (dense, bf16, VMEM),
            (square, bf16, VMEM),
            (dense, bf16, VMEM),
            (pairs, bf16, VMEM),
            (pairs, bf16, VMEM),
            ((2,) + square, f32, VMEM),
        ],
        [
            pltpu.VMEM((2,) + square, f32),
            pltpu.VMEM((2,) + square, f32),
            pltpu.VMEM((2,) + square, f32),
            pltpu.VMEM((2, PANEL, 2 * PANEL), f32),
            sems(7),
        ],
        20_000_000_000,
    )
    inverse_up = shifted(mine, -1, 0)
    inverse_right = shifted(mine, 0, -1)
    got_above = shifted(give_down, 1, 0)
    right, give_sym, give_cross = called(
        give_kernel,
        [(packed, VMEM), (down, VMEM), (flat, VMEM)],
        [(square, bf16, VMEM), (dense, bf16, VMEM), (square, bf16, VMEM)],
        [],
        1_000_000_000,
    )
    got_sym = shifted(give_sym, 0, 1)
    got_cross = shifted(give_cross, 0, 1)
    links_shape = ((2, 1, 4) + square, bf16, HBM)
    schur0, schur1, up, left, ready = called(
        own_kernel,
        [(packed, VMEM), (down, VMEM), (right, VMEM), (start, VMEM), (flat, VMEM), (upright, VMEM)],
        [
            (square, f32, VMEM), (square, f32, VMEM),
            (square, bf16, VMEM), (square, bf16, VMEM), ((3,) + square, bf16, VMEM),
        ],
        [pltpu.VMEM((2,) + square, bf16)],
        3_000_000_000,
    )
    schur0, ready, links = called(
        right_kernel,
        [
            (inverse_right, VMEM), (down_right, VMEM), (right_right, VMEM), (flat, VMEM),
            (schur0, VMEM), (up, VMEM), (right, VMEM), (ready, VMEM),
        ],
        [(square, f32, VMEM), ((2,) + square, bf16, VMEM), links_shape],
        [diagonal, pltpu.VMEM((3,) + square, bf16), sems(3)],
        2_000_000_000,
    )
    schur1, ready, links = called(
        below_kernel,
        [
            (inverse_up, VMEM), (down_up, VMEM), (right_up, VMEM), (left_up, VMEM),
            (upright, VMEM), (schur1, VMEM), (down, VMEM), (left, VMEM),
            (got_cross, VMEM), (ready, VMEM), (links, HBM),
        ],
        [(square, f32, VMEM), ((3,) + square, bf16, VMEM), links_shape],
        [diagonal, pltpu.VMEM((4,) + square, bf16), sems(2)],
        3_000_000_000,
        {10: 2},
    )
    schur_shape = ((2, 1) + square, f32, HBM)
    strips = sems(order // PANEL)
    schur, links = called(
        schur_odd_kernel,
        [(schur1, VMEM), (got_sym, VMEM), (ready, VMEM), (links, HBM)],
        [schur_shape, links_shape],
        [pltpu.VMEM(square, f32), sems(order // PANEL + 3)],
        300_000_000,
        {3: 1},
    )
    (schur,) = called(
        schur_even_kernel,
        [(schur0, VMEM), (got_above, VMEM), (schur, HBM)],
        [schur_shape],
        [pltpu.VMEM(square, f32), strips],
        300_000_000,
        {2: 0},
    )
    return (factor[:, None], schur, links)


def solution(mesh):
    in_specs = (
        P("row", "col", None, None),
        P("row", "col", None, None),
        P("row", "col", None, None),
    )
    out_specs = (
        P("row", "col", None, None),
        P("row", "col", None, None),
        P("row", "col", None, None, None),
    )
    return jax.shard_map(
        on_device, mesh=mesh, in_specs=in_specs, out_specs=out_specs, check_vma=False
    )
```
